256 devices in a mesh: lon: 32 (over y_lo, z, core), band: 8 (over y_hi, x).
Axes of the slice: x: 4, y: 4 (y_hi: 2, y_lo: 2; y = y_hi * 2 + y_lo), z: 8, core: 2. Of those that a mesh axis runs over, the one named last changes fastest.
Arguments:
- nest_field: float32 [32, 384, 9216], P(None, 'band', 'lon'), may hold values from -6 to 6
- nest_area: float32 [384, 9216], P('band', 'lon'), may hold values from 0.5 to 2
- parent_field: float32 [32, 128, 3072], P(None, 'band', 'lon'), may hold values from -6 to 6
- nest_offset: int32 [1], replicated, may hold values from 288 to 9215
- relax_rate: float32 [32], replicated, may hold values from 0.3 to 0.8
- zonal_coef: float32 [32], replicated, may hold values from 0.05 to 0.24
- merid_coef: float32 [32], replicated, may hold values from 0.05 to 0.24
Outputs:
- parent_out: float32 [32, 128, 3072], P(None, 'band', 'lon')
The draws below stay inside these ranges and needn't reach their ends.
All inputs are finite; a program needn't handle non-finite values.
Results may differ from the reference program's by a relative error of at most 0.000084.
Values sent between devices are 32-bit elements; how exact they have to be, the bound alone decides.
A program may use at most 64 MiB of HBM per device.

```python
import math
import jax
import jax.numpy as jnp

NXP = 3072
LV = 32
NS = 3
NYP = 128
NYN = 384
NXN = 9216
N_LON = 32


def block_levels(stream_key, shape, split, low, largest):
    def one(axis_at, blocks):
        draws = jax.random.uniform(jax.random.fold_in(jax.random.fold_in(stream_key, 6), axis_at), (blocks,), jnp.float32, low / len(split), largest / len(split))
        return jnp.repeat(jnp.exp(draws), shape[axis_at] // blocks).reshape((-1,) + (1,) * (len(shape) - axis_at - 1))

    level = one(*split[0])
    for cut in split[1:]:
        level = level * one(*cut)
    return level


def centred(key, shape, scale, bound, cuts=(), kind=jnp.bfloat16):
    factor_of = block_levels(key, shape, cuts, -0.22, 0.18) if cuts else 1.0
    result = jax.random.normal(key, shape, jnp.float32) * scale * factor_of
    return jnp.minimum(jnp.maximum(result, -bound), bound).astype(kind)


def setup_inputs(seed: int = 0) -> dict:
    streams_of = jax.random.split(jax.random.key(seed), 8)
    return {
        "nest_field": centred(streams_of[0], (LV, NYN, NXN), 1.0, 6.0, ((1, 8), (2, 32)), jnp.float32),
        "nest_area": jnp.clip(jnp.exp(math.log(2.0) - 1.3862944 * jax.random.uniform(streams_of[1], (NYN, NXN), jnp.float32) ** block_levels(streams_of[1], (NYN, NXN), ((0, 8), (1, 32)), -0.2, 0.2)), 0.5, 2.0),
        "parent_field": centred(streams_of[2], (LV, NYP, NXP), 1.0, 6.0, ((1, 8), (2, 32)), jnp.float32),
        "nest_offset": jax.random.randint(streams_of[3], (1,), 3 * NXP // N_LON, 3 * NXP).astype(jnp.int32),
        "relax_rate": jnp.clip(jax.random.uniform(streams_of[4], (LV,), jnp.float32, 0.3, 0.8), 0.3, 0.8),
        "zonal_coef": jnp.clip(jax.random.uniform(streams_of[5], (LV,), jnp.float32, 0.05, 0.24), 0.05, 0.24),
        "merid_coef": jnp.clip(jax.random.uniform(streams_of[6], (LV,), jnp.float32, 0.05, 0.24), 0.05, 0.24),
    }


def zonal_pass(field, coef):
    left = jnp.roll(field, 1, axis=2)
    right = jnp.roll(field, -1, axis=2)
    return field + coef[:, None, None] * (left - 2.0 * field + right)


def merid_pass(field, coef):
    padded = jnp.pad(field, ((0, 0), (1, 1), (0, 0)))
    return field + coef[:, None, None] * (padded[:, :-2] - 2.0 * field + padded[:, 2:])


def reference(nest_field, nest_area, parent_field, nest_offset, relax_rate, zonal_coef, merid_coef):
    offset_cells = nest_offset[0]
    stacked = jnp.concatenate([nest_field * nest_area[None], nest_area[None]], axis=0)
    planes = stacked.shape[0]
    row_sums = stacked.reshape(planes, NYP, 3, NXN).sum(axis=2)
    rolled = jnp.roll(row_sums, offset_cells, axis=2)
    cell_sums = rolled.reshape(planes, NYP, NXP, 3).sum(axis=3)
    restricted = cell_sums[:LV] / cell_sums[LV][None]
    field = parent_field + relax_rate[:, None, None] * (restricted - parent_field)
    for sweep in range(NS):
        field = zonal_pass(field, zonal_coef)
        field = merid_pass(field, merid_coef)
    return field
```

```python
import functools

import jax
import jax.numpy as jnp
from jax import lax
from jax.experimental import pallas as pl
from jax.experimental.pallas import tpu as pltpu
from jax.sharding import PartitionSpec as P

NS = 3
FRAME = 104
LANES = 128
CUT = 32
MESH = pl.DeviceIdType.MESH
VMEM = pl.BlockSpec(memory_space=pltpu.VMEM)
SMEM = pl.BlockSpec(memory_space=pltpu.SMEM)


def pieces(value):
    high = value.astype(jnp.bfloat16)
    rest = value - high.astype(jnp.float32)
    middle = rest.astype(jnp.bfloat16)
    low = (rest - middle.astype(jnp.float32)).astype(jnp.bfloat16)
    return high, middle, low


def product(left, right_pieces):
    total = None
    for piece in right_pieces:
        part = lax.dot_general(
            left, piece, (((1,), (1,)), ((), ())), preferred_element_type=jnp.float32
        )
        total = part if total is None else total + part
    return total


def restrict_kernel(
    offset, nest, area, parent, x_own, x_next, x_edge, p_edge, tiles, area_tiles, sums, plain, cells
):
    levels, width = 32, nest.shape[1]
    par_rows = parent.shape[0] // levels
    nest_rows = 3 * par_rows
    inner = lax.rem(offset[0], width)

    def selector(window):
        cols = lax.broadcasted_iota(jnp.int32, (LANES, width), 1)
        slot = lax.broadcasted_iota(jnp.int32, (LANES, width), 0) - NS + (width // 3) * window
        gap = cols + inner - 3 * slot
        return ((gap >= 0) & (gap < 3)).astype(jnp.float32).astype(jnp.bfloat16)

    chosen = [selector(window) for window in (0, 1, -1, 2)]
    spans = [(at, min(LANES, width - at)) for at in range(0, width, LANES)]
    for t, (at, span) in enumerate(spans):
        area_tiles[t, :, 0:span] = area[:, at : at + span]

        def weigh(level, carry, t=t, at=at, span=span):
            rows = pl.ds(pl.multiple_of(level * nest_rows, 8), nest_rows)
            tiles[t, rows, 0:span] = nest[rows, at : at + span] * area[:, at : at + span]
            return carry

        lax.fori_loop(0, levels, weigh, 0)
    plain[:, 0 : parent.shape[1]] = parent[...]
    area_sums = jnp.concatenate(
        [
            sum(area_tiles[t, pl.ds(i, par_rows, 3), :] for i in range(3))[:, :span]
            for t, (_, span) in enumerate(spans)
        ],
        axis=1,
    )
    area_pieces = pieces(area_sums)
    for target, at, pick in ((x_own, FRAME, 0), (x_next, 0, 1), (x_edge.at[0], 8, 2), (x_edge.at[1], 8, 3)):
        spread = sum(
            lax.dot_general(piece, chosen[pick], (((1,), (1,)), ((), ())), preferred_element_type=jnp.float32)
            for piece in area_pieces
        )
        target[at : at + 8, 0:LANES] = spread[0:8]
        target[at : at + 8, LANES : 2 * LANES] = spread[8:16]
        target[at : at + 8, 2 * LANES :] = jnp.zeros((8, target.shape[1] - 2 * LANES), jnp.float32)
    for r in range(par_rows):
        here = slice(levels * r, levels * (r + 1))
        for t, (at, span) in enumerate(spans):
            sums[here, at : at + span] = sum(
                tiles[t, pl.ds(3 * r + i, levels, nest_rows), :] for i in range(3)
            )[:, :span]
        cells[here, :] = plain[pl.ds(r, levels, par_rows), :]
    left = jnp.concatenate(
        [chosen[0][:FRAME], chosen[1][:FRAME], chosen[2][FRAME - 8 : FRAME], chosen[3][:8]], axis=0
    )
    block = 2 * LANES
    for start in range(0, levels * par_rows, block):
        here = slice(start, start + block)
        spread = product(left, pieces(sums[here, :]))
        x_own[:FRAME, here] = spread[:FRAME]
        x_next[8 : 8 + FRAME, here] = spread[FRAME : 2 * FRAME]
        x_edge[0, 0:8, here] = spread[2 * FRAME : 2 * FRAME + 8]
        x_edge[1, 0:8, here] = spread[2 * FRAME + 8 :]
    par_cols = parent.shape[1]
    edge_row = lax.broadcasted_iota(jnp.int32, (16, par_cols), 0)
    edge_col = lax.broadcasted_iota(jnp.int32, (16, par_cols), 1)
    wanted = jnp.where(edge_row < 8, edge_row, edge_row + par_cols - 16)
    ends = (edge_col == wanted).astype(jnp.float32).astype(jnp.bfloat16)
    p_edge[...] = product(ends, pieces(cells[:, 0:par_cols]))


def shift_kernel(
    steps, cut, n_lon, x_own, x_next, x_edge, p_edge, r_own, r_next, r_edge, q_edge, sent, came
):
    lon = lax.axis_index("lon")
    moves = [
        (steps, x_own.at[pl.ds(CUT * cut, FRAME + 8 - CUT * cut)], r_own.at[pl.ds(CUT * cut, FRAME + 8 - CUT * cut)]),
        (steps + 1, x_next.at[pl.ds(0, CUT * cut + CUT + 16)], r_next.at[pl.ds(0, CUT * cut + CUT + 16)]),
        (1, p_edge.at[pl.ds(8, 8)], q_edge.at[pl.ds(0, 8)]),
        (-1, p_edge.at[pl.ds(0, 8)], q_edge.at[pl.ds(8, 8)]),
    ]
    if cut == 0:
        moves.append((steps - 1, x_edge.at[0], r_edge))
    if CUT * (cut + 1) >= FRAME - 8:
        moves.append((steps + 2, x_edge.at[1], r_edge))
    moves = [(hop % n_lon, source, target) for hop, source, target in moves]
    barrier = pltpu.get_barrier_semaphore()
    far = [hop for hop, _, _ in moves if hop]
    for hop in far:
        pl.semaphore_signal(
            barrier, inc=1, device_id={"lon": lax.rem(lon + n_lon - hop, n_lon)}, device_id_type=MESH
        )
    pl.semaphore_wait(barrier, len(far))
    copies = []
    for i, (hop, source, target) in enumerate(moves):
        if hop:
            copy = pltpu.make_async_remote_copy(
                source, target, sent.at[i], came.at[i],
                device_id={"lon": lax.rem(lon + hop, n_lon)}, device_id_type=MESH,
            )
        else:
            copy = pltpu.make_async_copy(source, target, came.at[i])
        copy.start()
        copies.append(copy)
    for copy in copies:
        copy.wait()


def smooth_kernel(
    n_band, offset, r_own, r_next, r_edge, q_edge, parent, relax, zonal, merid, out,
    turned, coef, field, other, plain, sent, came,
):
    levels = 32
    par_rows = parent.shape[0] // levels
    par_cols = parent.shape[1]
    band = lax.axis_index("band")
    before, after = lax.rem(band + n_band - 1, n_band), lax.rem(band + 1, n_band)
    barrier = pltpu.get_barrier_semaphore()
    for near in (before, after):
        pl.semaphore_signal(barrier, inc=1, device_id={"band": near}, device_id_type=MESH)
    start = lax.rem(offset[0], 3 * par_cols) // 3
    first = start < CUT
    last = start >= par_cols - CUT
    shape = (FRAME, levels * par_rows)
    row = lax.broadcasted_iota(jnp.int32, shape, 0)
    none = jnp.zeros((8, levels * par_rows), jnp.float32)
    turned[0:FRAME, :] = jnp.where(row >= start + NS, r_own[0:FRAME, :], 0.0) + jnp.where(
        row <= start + NS, r_next[8 : 8 + FRAME, :], 0.0
    )
    turned[0:8, :] += jnp.where(last, r_edge[0:8, :], none)
    turned[FRAME - 8 : FRAME, :] += jnp.where(first, r_edge[0:8, :], none)
    turned[FRAME : FRAME + 8, :] = q_edge[8:16, :]
    turned[FRAME + 8 : LANES - 8, :] = jnp.zeros((LANES - 16 - FRAME, levels * par_rows), jnp.float32)
    turned[LANES - 8 :, :] = q_edge[0:8, :]
    zero = jnp.zeros((8, LANES), jnp.float32)
    inverse = []
    for half in range(2):
        at = slice(half * LANES, (half + 1) * LANES)
        extra = jnp.where(first | last, r_edge[8:16, at], zero)
        inverse.append(1.0 / (r_own[FRAME : FRAME + 8, at] + r_next[0:8, at] + extra))
    coef[...] = jnp.zeros_like(coef)
    coef[0:1, 0:levels] = relax[...]
    coef[1:2, 0:levels] = zonal[...]
    coef[2:3, 0:levels] = merid[...]
    columns = coef[...].T
    weight = [jnp.broadcast_to(columns[0:levels, k : k + 1], (levels, LANES)) for k in range(3)]
    plain[:, 0:par_cols] = parent[...]
    lane = lax.broadcasted_iota(jnp.int32, (levels, LANES), 1)
    per = LANES // levels
    for block in range(par_rows // per):
        natural = turned[:, LANES * block : LANES * (block + 1)].T
        for k in range(per):
            r = per * block + k
            got = natural[levels * k : levels * (k + 1), :]
            own = plain[pl.ds(r, levels, par_rows), :]
            base = jnp.where(
                lane < par_cols + NS,
                pltpu.roll(jnp.where(lane < par_cols, own, got), NS, 1),
                pltpu.roll(got, LANES + par_cols + NS - FRAME, 1),
            )
            scaled = got * inverse[r // 8][r % 8 : r % 8 + 1, :]
            at = levels * (NS + r)
            field[at : at + levels, :] = base + weight[0] * (scaled - base)
    pl.semaphore_wait(barrier, 2)
    size = levels * NS
    total = levels * par_rows
    copies = []
    for i, (near, source, target) in enumerate(((before, size, size + total), (after, total, 0))):
        copy = pltpu.make_async_remote_copy(
            field.at[pl.ds(source, size)], field.at[pl.ds(target, size)], sent.at[i], came.at[i],
            device_id={"band": near}, device_id_type=MESH,
        )
        copy.start()
        copies.append(copy)
    for copy in copies:
        copy.wait()
    rows = par_rows + 2 * NS

    def load(ref, r):
        value = ref[levels * r : levels * (r + 1), :]
        if r < NS:
            value = jnp.where(band > 0, value, 0.0)
        if r >= NS + par_rows:
            value = jnp.where(band < n_band - 1, value, 0.0)
        return value

    refs = [field, other]
    for sweep in range(NS):
        read, write = refs[sweep % 2], refs[1 - sweep % 2]
        zoned = {}
        for r in range(sweep, rows - sweep):
            value = load(read, r)
            zoned[r] = value + weight[1] * (
                pltpu.roll(value, 1, 1) - 2.0 * value + pltpu.roll(value, LANES - 1, 1)
            )
            if r >= sweep + 2:
                middle = zoned[r - 1]
                result = middle + weight[2] * (zoned[r - 2] - 2.0 * middle + zoned[r])
                if sweep < NS - 1:
                    write[levels * (r - 1) : levels * r, :] = result
                else:
                    plain[pl.ds(r - 1 - NS, levels, par_rows), :] = pltpu.roll(result, LANES - NS, 1)
    out[...] = plain[:, 0:par_cols]


def on_device(nest_field, nest_area, parent_field, nest_offset, relax_rate, zonal_coef, merid_coef):
    levels, par_rows, par_cols = parent_field.shape
    n_lon, n_band = lax.axis_size("lon"), lax.axis_size("band")
    width = nest_field.shape[2]
    total = levels * par_rows
    f32 = jnp.float32
    nest = nest_field.reshape(-1, width)
    parent = parent_field.reshape(total, par_cols)

    def shaped(*shape):
        return jax.ShapeDtypeStruct(shape, f32)

    sides = pl.pallas_call(
        restrict_kernel,
        name="restrict",
        out_shape=[shaped(FRAME + 8, total), shaped(FRAME + 8, total), shaped(2, 16, total), shaped(16, total)],
        in_specs=[SMEM, VMEM, VMEM, VMEM],
        out_specs=[VMEM] * 4,
        scratch_shapes=[
            pltpu.VMEM((-(-width // LANES), nest.shape[0], LANES), f32),
            pltpu.VMEM((-(-width // LANES), nest_area.shape[0], LANES), f32),
            pltpu.VMEM((total, width), f32),
            pltpu.VMEM((total, LANES), f32),
            pltpu.VMEM((total, LANES), f32),
        ],
    )(nest_offset, nest, nest_area, parent)

    def shift(place):
        steps, cut = place // (par_cols // CUT), place % (par_cols // CUT)
        return pl.pallas_call(
            functools.partial(shift_kernel, steps, cut, n_lon),
            name="shift%d" % place,
            out_shape=[shaped(FRAME + 8, total), shaped(FRAME + 8, total), shaped(16, total), shaped(16, total)],
            in_specs=[VMEM] * 4,
            out_specs=[VMEM] * 4,
            scratch_shapes=[pltpu.SemaphoreType.DMA((5,)), pltpu.SemaphoreType.DMA((5,))],
            compiler_params=pltpu.CompilerParams(collective_id=place, has_side_effects=True),
        )

    low = par_cols // CUT
    places = range(low, n_lon * low)
    place = nest_offset[0] // (3 * CUT) - low
    moved = lax.switch(place, [lambda *a, p=p: shift(p)(*a) for p in places], *sides)
    out = pl.pallas_call(
        functools.partial(smooth_kernel, n_band),
        name="smooth",
        out_shape=shaped(total, par_cols),
        in_specs=[SMEM] + [VMEM] * 8,
        out_specs=VMEM,
        scratch_shapes=[
            pltpu.VMEM((LANES, total), f32),
            pltpu.VMEM((LANES, LANES), f32),
            pltpu.VMEM((levels * (par_rows + 2 * NS), LANES), f32),
            pltpu.VMEM((levels * (par_rows + 2 * NS), LANES), f32),
            pltpu.VMEM((total, LANES), f32),
            pltpu.SemaphoreType.DMA((2,)),
            pltpu.SemaphoreType.DMA((2,)),
        ],
        compiler_params=pltpu.CompilerParams(collective_id=0, has_side_effects=True),
    )(
        nest_offset, *moved, parent,
        relax_rate.reshape(1, levels), zonal_coef.reshape(1, levels), merid_coef.reshape(1, levels),
    )
    return out.reshape(levels, par_rows, par_cols)


def solution(mesh):
    placed = (P(None, "band", "lon"), P("band", "lon"), P(None, "band", "lon"), P(), P(), P(), P())
    return jax.shard_map(
        on_device, mesh=mesh, in_specs=placed, out_specs=P(None, "band", "lon"), check_vma=False
    )
```

```python
import functools

import jax
import jax.numpy as jnp
from jax import lax
from jax.experimental import pallas as pl
from jax.experimental.pallas import tpu as pltpu
from jax.sharding import PartitionSpec as P

NS = 3
FRAME = 104
LANES = 128
MESH = pl.DeviceIdType.MESH
VMEM = pl.BlockSpec(memory_space=pltpu.VMEM)
SMEM = pl.BlockSpec(memory_space=pltpu.SMEM)


def pieces(value):
    high = value.astype(jnp.bfloat16)
    rest = value - high.astype(jnp.float32)
    middle = rest.astype(jnp.bfloat16)
    low = (rest - middle.astype(jnp.float32)).astype(jnp.bfloat16)
    return high, middle, low


def product(left, right_pieces):
    total = None
    for piece in right_pieces:
        part = lax.dot_general(
            left, piece, (((1,), (1,)), ((), ())), preferred_element_type=jnp.float32
        )
        total = part if total is None else total + part
    return total


def restrict_kernel(
    offset, nest, area, parent, x_own, x_next, x_edge, p_edge, p_rows,
    tiles, area_tiles, sums, plain, cells,
):
    levels, width = 32, nest.shape[1]
    par_rows = parent.shape[0] // levels
    nest_rows = 3 * par_rows
    inner = lax.rem(offset[0], width)

    def selector(window):
        cols = lax.broadcasted_iota(jnp.int32, (LANES, width), 1)
        slot = lax.broadcasted_iota(jnp.int32, (LANES, width), 0) - NS + (width // 3) * window
        gap = cols + inner - 3 * slot
        return ((gap >= 0) & (gap < 3)).astype(jnp.float32).astype(jnp.bfloat16)

    chosen = [selector(window) for window in (0, 1, -1, 2)]
    spans = [(at, min(LANES, width - at)) for at in range(0, width, LANES)]
    for t, (at, span) in enumerate(spans):
        area_tiles[t, :, 0:span] = area[:, at : at + span]

        def weigh(level, carry, t=t, at=at, span=span):
            rows = pl.ds(pl.multiple_of(level * nest_rows, 8), nest_rows)
            tiles[t, rows, 0:span] = nest[rows, at : at + span] * area[:, at : at + span]
            return carry

        lax.fori_loop(0, levels, weigh, 0)
    plain[:, 0 : parent.shape[1]] = parent[...]
    area_sums = jnp.concatenate(
        [
            sum(area_tiles[t, pl.ds(i, par_rows, 3), :] for i in range(3))[:, :span]
            for t, (_, span) in enumerate(spans)
        ],
        axis=1,
    )
    area_pieces = pieces(area_sums)
    per = LANES // levels
    blocks = par_rows // per
    for target, at, pick in ((x_own, FRAME, 0), (x_next, FRAME, 1), (x_edge.at[0], 8, 2), (x_edge.at[1], 8, 3)):
        spread = sum(
            lax.dot_general(piece, chosen[pick], (((1,), (1,)), ((), ())), preferred_element_type=jnp.float32)
            for piece in area_pieces
        )
        for block in range(blocks):
            tile = 8 * (per * block // 8)
            target[block, at : at + 8, :] = spread[tile : tile + 8]
    for r in range(par_rows):
        here = slice(levels * r, levels * (r + 1))
        for t, (at, span) in enumerate(spans):
            sums[here, at : at + span] = sum(
                tiles[t, pl.ds(3 * r + i, levels, nest_rows), :] for i in range(3)
            )[:, :span]
        cells[here, :] = plain[pl.ds(r, levels, par_rows), :]
    left = jnp.concatenate(
        [chosen[0][:FRAME], chosen[1][:FRAME], chosen[2][FRAME - 8 : FRAME], chosen[3][:8]], axis=0
    )
    for pair in range(0, blocks, 2):
        spread = product(left, pieces(sums[LANES * pair : LANES * (pair + 2), :]))
        for block in (pair, pair + 1):
            here = slice(LANES * (block - pair), LANES * (block - pair + 1))
            x_own[block, :FRAME, :] = spread[:FRAME, here]
            x_next[block, :FRAME, :] = spread[FRAME : 2 * FRAME, here]
            x_edge[0, block, 0:8, :] = spread[2 * FRAME : 2 * FRAME + 8, here]
            x_edge[1, block, 0:8, :] = spread[2 * FRAME + 8 :, here]
    par_cols = parent.shape[1]
    edge_row = lax.broadcasted_iota(jnp.int32, (16, par_cols), 0)
    edge_col = lax.broadcasted_iota(jnp.int32, (16, par_cols), 1)
    wanted = jnp.where(edge_row < 8, edge_row, edge_row + par_cols - 16)
    ends = (edge_col == wanted).astype(jnp.float32).astype(jnp.bfloat16)
    ends_of = product(ends, pieces(cells[:, 0:par_cols]))
    for block in range(blocks):
        p_edge[block, :, :] = ends_of[:, LANES * block : LANES * (block + 1)]
    p_rows[0, :, :] = cells[0 : levels * NS, :]
    p_rows[1, :, :] = cells[levels * (par_rows - NS) :, :]


def route_kernel(
    steps, n_lon, n_band, x_own, x_next, x_edge, p_edge, p_rows,
    main, halo, q_edge, q_corner, q_rows, r_next, r_edge, total, sent, came,
):
    blocks = x_own.shape[0]
    end, mid = blocks - 1, pl.ds(1, blocks - 2)
    low, high = pl.ds(0, 8), pl.ds(8, 8)
    moves = [
        (1, 0, x_next.at[0], r_next.at[0]),
        (-1, 0, x_edge.at[0], r_edge.at[0]),
        (2, 0, x_edge.at[1], r_edge.at[1]),
        (1, 0, x_next.at[end], r_next.at[end]),
        (1, 0, x_next.at[mid], r_next.at[mid]),
        (1, 0, p_edge.at[:, high], q_edge.at[:, low]),
        (-1, 0, p_edge.at[:, low], q_edge.at[:, high]),
        (0, 1, p_rows.at[1], q_rows.at[0]),
        (0, -1, p_rows.at[0], q_rows.at[1]),
        (1, 1, p_edge.at[end, high], q_corner.at[0, low]),
        (-1, 1, p_edge.at[end, low], q_corner.at[0, high]),
        (1, -1, p_edge.at[0, high], q_corner.at[1, low]),
        (-1, -1, p_edge.at[0, low], q_corner.at[1, high]),
        (steps, 0, total.at[0], main.at[0]),
        (steps, 0, total.at[end], main.at[end]),
        (steps, 0, total.at[mid], main.at[mid]),
        (0, -1, main.at[0], halo.at[1]),
        (0, 1, main.at[end], halo.at[0]),
    ]

    def device(east, north):
        return {
            "lon": lax.rem(lax.axis_index("lon") + n_lon + east, n_lon),
            "band": lax.rem(lax.axis_index("band") + n_band + north, n_band),
        }

    copies = [
        pltpu.make_async_remote_copy(
            source, target, sent.at[i], came.at[i], device_id=device(east, north), device_id_type=MESH
        )
        for i, (east, north, source, target) in enumerate(moves)
    ]
    barrier = pltpu.get_barrier_semaphore()
    near = sorted({(east % n_lon, north) for east, north, _, _ in moves})
    for east, north in near:
        pl.semaphore_signal(barrier, inc=1, device_id=device(-east, -north), device_id_type=MESH)
    pl.semaphore_wait(barrier, len(near))
    for copy in copies[:13]:
        copy.start()

    def add(block):
        total[block] = x_own[block] + r_next[block]
        total[block, 0:8, :] += r_edge[1, block, 0:8, :]
        total[block, FRAME - 8 : FRAME, :] += r_edge[0, block, 0:8, :]
        total[block, FRAME:, :] += r_edge[0, block, 8:, :] + r_edge[1, block, 8:, :]

    for i in (0, 1, 2):
        copies[i].wait_recv()
    add(0)
    copies[13].start()
    copies[3].wait_recv()
    add(end)
    copies[14].start()
    copies[4].wait_recv()
    for block in range(1, end):
        add(block)
    copies[15].start()
    copies[13].wait_recv()
    copies[16].start()
    copies[14].wait_recv()
    copies[17].start()
    for i in (5, 6, 7, 8, 9, 10, 11, 12, 15, 16, 17):
        copies[i].wait_recv()
    for copy in copies:
        copy.wait_send()


def smooth_kernel(
    n_band, main, halo, q_edge, q_corner, q_rows, parent, relax, zonal, merid, out,
    coef, field, other, plain,
):
    levels = 32
    par_rows = parent.shape[0] // levels
    par_cols = parent.shape[1]
    band = lax.axis_index("band")
    coef[...] = jnp.zeros_like(coef)
    coef[0:1, 0:levels] = relax[...]
    coef[1:2, 0:levels] = zonal[...]
    coef[2:3, 0:levels] = merid[...]
    across = coef[...].T
    weight = [jnp.broadcast_to(across[0:levels, k : k + 1], (levels, LANES)) for k in range(3)]
    plain[:, 0:par_cols] = parent[...]
    lane = lax.broadcasted_iota(jnp.int32, (levels, LANES), 1)
    per = LANES // levels
    gap = jnp.zeros((LANES - 16 - FRAME, LANES), jnp.float32)

    def blend(sums, edges, first, wanted):
        inverse = 1.0 / sums[FRAME:]
        natural = jnp.concatenate([sums[:FRAME], edges[8:16], gap, edges[0:8]], axis=0).T
        for k, own, r in wanted:
            area_row = inverse[first + k : first + k + 1, :]
            got = natural[levels * k : levels * (k + 1), :]
            base = jnp.where(
                lane < par_cols + NS,
                pltpu.roll(jnp.where(lane < par_cols, own(), got), NS, 1),
                pltpu.roll(got, LANES + par_cols + NS - FRAME, 1),
            )
            field[levels * r : levels * (r + 1), :] = base + weight[0] * (got * area_row - base)

    blend(
        halo[0], q_corner[0], 8 - per,
        [
            (per - NS + k, lambda k=k: q_rows[0, levels * k : levels * (k + 1), :], k)
            for k in range(NS)
        ],
    )
    for block in range(par_rows // per):
        blend(
            main[block], q_edge[block], per * block % 8,
            [
                (r % per, lambda r=r: plain[pl.ds(r, levels, par_rows), :], NS + r)
                for r in range(per * block, per * (block + 1))
            ],
        )
    blend(
        halo[1], q_corner[1], 0,
        [
            (k, lambda k=k: q_rows[1, levels * k : levels * (k + 1), :], NS + par_rows + k)
            for k in range(NS)
        ],
    )
    rows = par_rows + 2 * NS

    def load(ref, r):
        value = ref[levels * r : levels * (r + 1), :]
        if r < NS:
            value = jnp.where(band > 0, value, 0.0)
        if r >= NS + par_rows:
            value = jnp.where(band < n_band - 1, value, 0.0)
        return value

    refs = [field, other]
    for sweep in range(NS):
        read, write = refs[sweep % 2], refs[1 - sweep % 2]
        zoned = {}
        for r in range(sweep, rows - sweep):
            value = load(read, r)
            zoned[r] = value + weight[1] * (
                pltpu.roll(value, 1, 1) - 2.0 * value + pltpu.roll(value, LANES - 1, 1)
            )
            if r >= sweep + 2:
                middle = zoned[r - 1]
                result = middle + weight[2] * (zoned[r - 2] - 2.0 * middle + zoned[r])
                if sweep < NS - 1:
                    write[levels * (r - 1) : levels * r, :] = result
                else:
                    plain[pl.ds(r - 1 - NS, levels, par_rows), :] = pltpu.roll(result, LANES - NS, 1)
    out[...] = plain[:, 0:par_cols]


def on_device(nest_field, nest_area, parent_field, nest_offset, relax_rate, zonal_coef, merid_coef):
    levels, par_rows, par_cols = parent_field.shape
    n_lon, n_band = lax.axis_size("lon"), lax.axis_size("band")
    width = nest_field.shape[2]
    total = levels * par_rows
    f32 = jnp.float32
    nest = nest_field.reshape(-1, width)
    parent = parent_field.reshape(total, par_cols)

    def shaped(*shape):
        return jax.ShapeDtypeStruct(shape, f32)

    per_block = total // LANES
    sides = pl.pallas_call(
        restrict_kernel,
        name="restrict",
        out_shape=[
            shaped(per_block, FRAME + 8, LANES),
            shaped(per_block, FRAME + 8, LANES),
            shaped(2, per_block, 16, LANES),
            shaped(per_block, 16, LANES),
            shaped(2, levels * NS, LANES),
        ],
        in_specs=[SMEM, VMEM, VMEM, VMEM],
        out_specs=[VMEM] * 5,
        scratch_shapes=[
            pltpu.VMEM((-(-width // LANES), nest.shape[0], LANES), f32),
            pltpu.VMEM((-(-width // LANES), nest_area.shape[0], LANES), f32),
            pltpu.VMEM((total, width), f32),
            pltpu.VMEM((total, LANES), f32),
            pltpu.VMEM((total, LANES), f32),
        ],
    )(nest_offset, nest, nest_area, parent)

    def route(steps):
        return pl.pallas_call(
            functools.partial(route_kernel, steps, n_lon, n_band),
            name="route%d" % steps,
            out_shape=[
                shaped(per_block, FRAME + 8, LANES),
                shaped(2, FRAME + 8, LANES),
                shaped(per_block, 16, LANES),
                shaped(2, 16, LANES),
                shaped(2, levels * NS, LANES),
            ],
            in_specs=[VMEM] * 5,
            out_specs=[VMEM] * 5,
            scratch_shapes=[
                pltpu.VMEM((per_block, FRAME + 8, LANES), f32),
                pltpu.VMEM((2, per_block, 16, LANES), f32),
                pltpu.VMEM((per_block, FRAME + 8, LANES), f32),
                pltpu.SemaphoreType.DMA((18,)),
                pltpu.SemaphoreType.DMA((18,)),
            ],
            compiler_params=pltpu.CompilerParams(collective_id=steps, has_side_effects=True),
        )

    routes = [lambda *values, steps=steps: route(steps)(*values) for steps in range(1, n_lon)]
    moved = lax.switch(nest_offset[0] // width - 1, routes, *sides)
    rows = levels * (par_rows + 2 * NS)
    out = pl.pallas_call(
        functools.partial(smooth_kernel, n_band),
        name="smooth",
        out_shape=shaped(total, par_cols),
        in_specs=[VMEM] * 9,
        out_specs=VMEM,
        scratch_shapes=[
            pltpu.VMEM((LANES, LANES), f32),
            pltpu.VMEM((rows, LANES), f32),
            pltpu.VMEM((rows, LANES), f32),
            pltpu.VMEM((total, LANES), f32),
        ],
    )(
        *moved, parent,
        relax_rate.reshape(1, levels), zonal_coef.reshape(1, levels), merid_coef.reshape(1, levels),
    )
    return out.reshape(levels, par_rows, par_cols)


def solution(mesh):
    placed = (P(None, "band", "lon"), P("band", "lon"), P(None, "band", "lon"), P(), P(), P(), P())
    return jax.shard_map(
        on_device, mesh=mesh, in_specs=placed, out_specs=P(None, "band", "lon"), check_vma=False
    )
```

```python
import functools

import jax
import jax.numpy as jnp
from jax import lax
from jax.experimental import pallas as pl
from jax.experimental.pallas import tpu as pltpu
from jax.sharding import PartitionSpec as P

NS = 3
FRAME = 104
LANES = 128
MESH = pl.DeviceIdType.MESH
VMEM = pl.BlockSpec(memory_space=pltpu.VMEM)
SMEM = pl.BlockSpec(memory_space=pltpu.SMEM)


def pieces(value, count):
    found = []
    for _ in range(count):
        piece = value.astype(jnp.bfloat16)
        value = value - piece.astype(jnp.float32)
        found.append(piece)
    return found


def product(left_pieces, right_pieces):
    total = None
    for left in left_pieces:
        for right in right_pieces:
            part = lax.dot_general(
                left, right, (((1,), (1,)), ((), ())), preferred_element_type=jnp.float32
            )
            total = part if total is None else total + part
    return total


def route_kernel(
    steps, n_lon, n_band, offset, nest, area, parent, relax, zonal, merid,
    main, halo, q_edge, q_corner, q_rows, cells, weights,
    nest_in, area_in, parent_in, relax_in, zonal_in, merid_in, tiles, area_tiles, sums, plain, chosen,
    x_own, x_next, x_edge, p_edge, r_next, r_edge, total, sent, came, read,
):
    levels, width, par_cols = 32, nest.shape[1], parent.shape[1]
    par_rows = parent.shape[0] // levels
    nest_rows = 3 * par_rows
    per = LANES // levels
    blocks = par_rows // per
    end, mid = blocks - 1, pl.ds(1, blocks - 2)
    low, high = pl.ds(0, 8), pl.ds(8, 8)
    columns = levels * par_rows
    moves = [
        (1, 0, x_next.at[0], r_next.at[0]),
        (-1, 0, x_edge.at[0], r_edge.at[0]),
        (2, 0, x_edge.at[1], r_edge.at[1]),
        (1, 0, x_next.at[end], r_next.at[end]),
        (1, 0, x_next.at[mid], r_next.at[mid]),
        (1, 0, p_edge.at[:, high], q_edge.at[:, low]),
        (-1, 0, p_edge.at[:, low], q_edge.at[:, high]),
        (0, 1, cells.at[pl.ds(columns - levels * NS, levels * NS)], q_rows.at[0]),
        (0, -1, cells.at[pl.ds(0, levels * NS)], q_rows.at[1]),
        (1, 1, p_edge.at[end, high], q_corner.at[0, low]),
        (-1, 1, p_edge.at[end, low], q_corner.at[0, high]),
        (1, -1, p_edge.at[0, high], q_corner.at[1, low]),
        (-1, -1, p_edge.at[0, low], q_corner.at[1, high]),
        (steps, 0, total.at[0], main.at[0]),
        (steps, 0, total.at[end], main.at[end]),
        (steps, 0, total.at[mid], main.at[mid]),
        (0, -1, main.at[0], halo.at[1]),
        (0, 1, main.at[end], halo.at[0]),
    ]

    def device(east, north):
        return {
            "lon": lax.rem(lax.axis_index("lon") + n_lon + east, n_lon),
            "band": lax.rem(lax.axis_index("band") + n_band + north, n_band),
        }

    barrier = pltpu.get_barrier_semaphore()
    near = sorted({(east % n_lon, north) for east, north, _, _ in moves})
    for east, north in near:
        pl.semaphore_signal(barrier, inc=1, device_id=device(-east, -north), device_id_type=MESH)

    reads = [
        pltpu.make_async_copy(source, target, read.at[i])
        for i, (source, target) in enumerate(
            ((area, area_in), (parent, parent_in), (relax, relax_in), (zonal, zonal_in), (merid, merid_in))
        )
    ]
    parts = 4
    rows_of = nest.shape[0] // parts

    def nest_part(i):
        here = pl.ds(pl.multiple_of(i * rows_of, 8), rows_of)
        return pltpu.make_async_copy(nest.at[here], nest_in.at[here], read.at[len(reads) + i])

    reads[0].start()
    for i in range(parts):
        nest_part(i).start()
    for copy in reads[1:]:
        copy.start()

    shape = (2 * FRAME + 16, width)
    row = lax.broadcasted_iota(jnp.int32, shape, 0)
    shift = jnp.where(
        row < FRAME,
        NS,
        jnp.where(
            row < 2 * FRAME,
            FRAME + NS - par_cols,
            jnp.where(row < 2 * FRAME + 8, FRAME + 8 + NS + par_cols, 2 * FRAME + 8 + NS - 2 * par_cols),
        ),
    )
    gap = lax.broadcasted_iota(jnp.int32, shape, 1) + lax.rem(offset[0], width) - 3 * (row - shift)
    chosen[...] = ((gap >= 0) & (gap < 3)).astype(jnp.float32).astype(jnp.bfloat16)

    spans = [(at, min(LANES, width - at)) for at in range(0, width, LANES)]
    reads[0].wait()
    for t, (at, span) in enumerate(spans):
        area_tiles[t, :, 0:span] = area_in[:, at : at + span]
    area_sums = jnp.concatenate(
        [
            sum(area_tiles[t, pl.ds(i, par_rows, 3), :] for i in range(3))[:, :span]
            for t, (_, span) in enumerate(spans)
        ],
        axis=1,
    )
    spread = product(pieces(area_sums, 3), [chosen[...]])
    spread = jnp.concatenate([spread, jnp.zeros((par_rows, 2 * LANES - shape[0]), jnp.float32)], axis=1)
    lane = lax.broadcasted_iota(jnp.int32, (par_rows, LANES), 1)
    zero = jnp.zeros((par_rows, LANES), jnp.float32)

    def window(start, first, count):
        turned = pltpu.roll(spread, (first - start) % (2 * LANES), 1)[:, :LANES]
        return jnp.where((lane >= first) & (lane < first + count), turned, zero)

    for target, at, here in (
        (x_own, FRAME, window(0, 0, FRAME)),
        (x_next, FRAME, window(FRAME, 0, FRAME)),
        (x_edge.at[0], 8, window(2 * FRAME, FRAME - 8, 8)),
        (x_edge.at[1], 8, window(2 * FRAME + 8, 0, 8)),
    ):
        for block in range(blocks):
            tile = 8 * (per * block // 8)
            target[block, at : at + 8, :] = here[tile : tile + 8]

    def weigh_part(i, carry):
        nest_part(i).wait()

        def weigh(level, inside):
            rows = pl.ds(pl.multiple_of(i * rows_of + level * nest_rows, 8), nest_rows)
            for t, (at, span) in enumerate(spans):
                tiles[t, rows, 0:span] = nest_in[rows, at : at + span] * area_in[:, at : at + span]
            return inside

        return lax.fori_loop(0, levels // parts, weigh, carry)

    lax.fori_loop(0, parts, weigh_part, 0)
    for copy in reads[1:]:
        copy.wait()
    plain[:, 0:par_cols] = parent_in[...]

    def gather(r, carry):
        here = pl.ds(pl.multiple_of(levels * r, levels), levels)
        for t, (at, span) in enumerate(spans):
            sums[here, at : at + span] = sum(
                tiles[t, pl.ds(3 * r + i, levels, nest_rows), :] for i in range(3)
            )[:, :span]
        cells[here, :] = plain[pl.ds(r, levels, par_rows), :]
        return carry

    lax.fori_loop(0, par_rows, gather, 0)
    edge_row = lax.broadcasted_iota(jnp.int32, (16, par_cols), 0)
    edge_col = lax.broadcasted_iota(jnp.int32, (16, par_cols), 1)
    wanted = jnp.where(edge_row < 8, edge_row, edge_row + par_cols - 16)
    ends = (edge_col == wanted).astype(jnp.float32).astype(jnp.bfloat16)

    def spread_pair(pair, carry):
        here = pl.ds(pl.multiple_of(2 * LANES * pair, 2 * LANES), 2 * LANES)
        spread = product([chosen[...]], pieces(sums[here, :], 2))
        outer = product([ends], pieces(cells[here, 0:par_cols], 3))
        for k in range(2):
            block, part = 2 * pair + k, slice(LANES * k, LANES * (k + 1))
            x_next[block, :FRAME, :] = spread[FRAME : 2 * FRAME, part]
            x_own[block, :FRAME, :] = spread[:FRAME, part]
            x_edge[0, block, 0:8, :] = spread[2 * FRAME : 2 * FRAME + 8, part]
            x_edge[1, block, 0:8, :] = spread[2 * FRAME + 8 :, part]
            p_edge[block, :, :] = outer[:, part]
        return carry

    lax.fori_loop(0, blocks // 2, spread_pair, 0)

    copies = [
        pltpu.make_async_remote_copy(
            source, target, sent.at[i], came.at[i], device_id=device(east, north), device_id_type=MESH
        )
        for i, (east, north, source, target) in enumerate(moves)
    ]
    pl.semaphore_wait(barrier, len(near))
    for copy in copies[:13]:
        copy.start()
    for k, values in enumerate((relax_in, zonal_in, merid_in)):
        upright = jnp.broadcast_to(values[...], (LANES, levels)).T
        weights[levels * k : levels * (k + 1), :] = upright

    def add(block):
        total[block] = x_own[block] + r_next[block]
        total[block, 0:8, :] += r_edge[1, block, 0:8, :]
        total[block, FRAME - 8 : FRAME, :] += r_edge[0, block, 0:8, :]
        total[block, FRAME:, :] += r_edge[0, block, 8:, :] + r_edge[1, block, 8:, :]

    for i in (0, 1, 2):
        copies[i].wait_recv()
    add(0)
    copies[13].start()
    copies[3].wait_recv()
    add(end)
    copies[14].start()
    copies[4].wait_recv()
    for block in range(1, end):
        add(block)
    copies[15].start()
    copies[13].wait_recv()
    copies[16].start()
    copies[14].wait_recv()
    copies[17].start()
    for i in (5, 6, 7, 8, 9, 10, 11, 12, 15, 16, 17):
        copies[i].wait_recv()
    for copy in copies:
        copy.wait_send()


def smooth_kernel(
    n_band, main, halo, q_edge, q_corner, q_rows, cells, weights, out, field, other, plain
):
    levels = 32
    par_rows = cells.shape[0] // levels
    par_cols = out.shape[1]
    band = lax.axis_index("band")
    weight = [weights[levels * k : levels * (k + 1), :] for k in range(3)]
    lane = lax.broadcasted_iota(jnp.int32, (levels, LANES), 1)
    per = LANES // levels
    gap = jnp.zeros((LANES - 16 - FRAME, LANES), jnp.float32)

    def blend(sums, edges, first, wanted):
        inverse = 1.0 / sums[FRAME:]
        natural = jnp.concatenate([sums[:FRAME], edges[8:16], gap, edges[0:8]], axis=0).T
        for k, own, r in wanted:
            area_row = inverse[first + k : first + k + 1, :]
            got = natural[levels * k : levels * (k + 1), :]
            base = jnp.where(
                lane < par_cols + NS,
                pltpu.roll(jnp.where(lane < par_cols, own(), got), NS, 1),
                pltpu.roll(got, LANES + par_cols + NS - FRAME, 1),
            )
            field[levels * r : levels * (r + 1), :] = base + weight[0] * (got * area_row - base)

    blend(
        halo[0], q_corner[0], 8 - per,
        [
            (per - NS + k, lambda k=k: q_rows[0, levels * k : levels * (k + 1), :], k)
            for k in range(NS)
        ],
    )
    for block in range(par_rows // per):
        blend(
            main[block], q_edge[block], per * block % 8,
            [
                (r % per, lambda r=r: cells[levels * r : levels * (r + 1), :], NS + r)
                for r in range(per * block, per * (block + 1))
            ],
        )
    blend(
        halo[1], q_corner[1], 0,
        [
            (k, lambda k=k: q_rows[1, levels * k : levels * (k + 1), :], NS + par_rows + k)
            for k in range(NS)
        ],
    )
    rows = par_rows + 2 * NS

    def load(ref, r):
        value = ref[levels * r : levels * (r + 1), :]
        if r < NS:
            value = jnp.where(band > 0, value, 0.0)
        if r >= NS + par_rows:
            value = jnp.where(band < n_band - 1, value, 0.0)
        return value

    refs = [field, other]
    for sweep in range(NS):
        read, write = refs[sweep % 2], refs[1 - sweep % 2]
        zoned = {}
        for r in range(sweep, rows - sweep):
            value = load(read, r)
            zoned[r] = value + weight[1] * (
                pltpu.roll(value, 1, 1) - 2.0 * value + pltpu.roll(value, LANES - 1, 1)
            )
            if r >= sweep + 2:
                middle = zoned[r - 1]
                result = middle + weight[2] * (zoned[r - 2] - 2.0 * middle + zoned[r])
                if sweep < NS - 1:
                    write[levels * (r - 1) : levels * r, :] = result
                else:
                    plain[pl.ds(r - 1 - NS, levels, par_rows), :] = pltpu.roll(result, LANES - NS, 1)
    out[...] = plain[:, 0:par_cols]


def on_device(nest_field, nest_area, parent_field, nest_offset, relax_rate, zonal_coef, merid_coef):
    levels, par_rows, par_cols = parent_field.shape
    n_lon, n_band = lax.axis_size("lon"), lax.axis_size("band")
    width = nest_field.shape[2]
    total = levels * par_rows
    f32 = jnp.float32
    nest = nest_field.reshape(-1, width)
    parent = parent_field.reshape(total, par_cols)

    def shaped(*shape):
        return jax.ShapeDtypeStruct(shape, f32)

    blocks = total // LANES
    spans = -(-width // LANES)

    def route(steps):
        return pl.pallas_call(
            functools.partial(route_kernel, steps, n_lon, n_band),
            name="route%d" % steps,
            out_shape=[
                shaped(blocks, FRAME + 8, LANES),
                shaped(2, FRAME + 8, LANES),
                shaped(blocks, 16, LANES),
                shaped(2, 16, LANES),
                shaped(2, levels * NS, LANES),
                shaped(total, LANES),
                shaped(3 * levels, LANES),
            ],
            in_specs=[SMEM] + [pl.BlockSpec(memory_space=pl.ANY)] * 6,
            out_specs=[VMEM] * 7,
            scratch_shapes=[
                pltpu.VMEM(nest.shape, f32),
                pltpu.VMEM(nest_area.shape, f32),
                pltpu.VMEM(parent.shape, f32),
                pltpu.VMEM((1, levels), f32),
                pltpu.VMEM((1, levels), f32),
                pltpu.VMEM((1, levels), f32),
                pltpu.VMEM((spans, nest.shape[0], LANES), f32),
                pltpu.VMEM((spans, nest_area.shape[0], LANES), f32),
                pltpu.VMEM((total, width), f32),
                pltpu.VMEM((total, LANES), f32),
                pltpu.VMEM((2 * FRAME + 16, width), jnp.bfloat16),
                pltpu.VMEM((blocks, FRAME + 8, LANES), f32),
                pltpu.VMEM((blocks, FRAME + 8, LANES), f32),
                pltpu.VMEM((2, blocks, 16, LANES), f32),
                pltpu.VMEM((blocks, 16, LANES), f32),
                pltpu.VMEM((blocks, FRAME + 8, LANES), f32),
                pltpu.VMEM((2, blocks, 16, LANES), f32),
                pltpu.VMEM((blocks, FRAME + 8, LANES), f32),
                pltpu.SemaphoreType.DMA((18,)),
                pltpu.SemaphoreType.DMA((18,)),
                pltpu.SemaphoreType.DMA((9,)),
            ],
            compiler_params=pltpu.CompilerParams(collective_id=steps, has_side_effects=True),
        )

    routes = [lambda *values, steps=steps: route(steps)(*values) for steps in range(1, n_lon)]
    moved = lax.switch(
        nest_offset[0] // width - 1,
        routes,
        nest_offset, nest, nest_area, parent,
        relax_rate.reshape(1, levels), zonal_coef.reshape(1, levels), merid_coef.reshape(1, levels),
    )
    rows = levels * (par_rows + 2 * NS)
    out = pl.pallas_call(
        functools.partial(smooth_kernel, n_band),
        name="smooth",
        out_shape=shaped(total, par_cols),
        in_specs=[VMEM] * 7,
        out_specs=VMEM,
        scratch_shapes=[
            pltpu.VMEM((rows, LANES), f32),
            pltpu.VMEM((rows, LANES), f32),
            pltpu.VMEM((total, LANES), f32),
        ],
    )(*moved)
    return out.reshape(levels, par_rows, par_cols)


def solution(mesh):
    placed = (P(None, "band", "lon"), P("band", "lon"), P(None, "band", "lon"), P(), P(), P(), P())
    return jax.shard_map(
        on_device, mesh=mesh, in_specs=placed, out_specs=P(None, "band", "lon"), check_vma=False
    )
```

```python
import functools

import jax
import jax.numpy as jnp
from jax import lax
from jax.experimental import pallas as pl
from jax.experimental.pallas import tpu as pltpu
from jax.sharding import PartitionSpec as P

NS = 3
FRAME = 104
LANES = 128
RING = 8
LIGHT = 2
HALF = 56
MESH = pl.DeviceIdType.MESH
VMEM = pl.BlockSpec(memory_space=pltpu.VMEM)
SMEM = pl.BlockSpec(memory_space=pltpu.SMEM)


def pieces(value, count):
    found = []
    for _ in range(count):
        piece = value.astype(jnp.bfloat16)
        value = value - piece.astype(jnp.float32)
        found.append(piece)
    return found


def product(left_pieces, right_pieces):
    total = None
    for left in left_pieces:
        for right in right_pieces:
            part = lax.dot_general(
                left, right, (((1,), (1,)), ((), ())), preferred_element_type=jnp.float32
            )
            total = part if total is None else total + part
    return total


def route_kernel(
    steps, n_lon, n_band, offset, nest, area, parent, relax, zonal, merid,
    main, halo, q_edge, q_corner, q_rows, cells, weights,
    nest_in, area_in, parent_in, relax_in, zonal_in, merid_in, tiles, area_tiles, sums, plain, chosen,
    x_own, x_side, p_edge, r_side, total, sent, came, read,
):
    levels, width, par_cols = 32, nest.shape[1], parent.shape[1]
    par_rows = parent.shape[0] // levels
    nest_rows = 3 * par_rows
    per = LANES // levels
    blocks = par_rows // per
    end, mid = blocks - 1, pl.ds(1, blocks - 2)
    low, high = pl.ds(0, 8), pl.ds(8, 8)
    columns = levels * par_rows
    hops = [(steps + core) // 2 % RING for core in range(2)]
    load = sum(min(hop, RING - hop) for hop in hops)
    light = load <= LIGHT
    away = steps % n_lon
    put = total if away else main
    moves = {}
    for k, east in enumerate((1, -1)):
        moves["carry%d" % k] = (east, 0, x_side.at[k, 0], r_side.at[k, 0])
    for k, east in enumerate((1, -1)):
        moves["carry%d" % (2 + k)] = (east, 0, x_side.at[k, end], r_side.at[k, end])
    for k, east in enumerate((1, -1)):
        moves["carry%d" % (4 + k)] = (east, 0, x_side.at[k, mid], r_side.at[k, mid])
    moves.update(
        {
            "edge0": (1, 0, p_edge.at[:, high], q_edge.at[:, low]),
            "edge1": (-1, 0, p_edge.at[:, low], q_edge.at[:, high]),
            "row0": (0, 1, cells.at[pl.ds(columns - levels * NS, levels * NS)], q_rows.at[0]),
            "row1": (0, -1, cells.at[pl.ds(0, levels * NS)], q_rows.at[1]),
            "corner0": (0, 1, q_edge.at[end], q_corner.at[0]),
            "corner1": (0, -1, q_edge.at[0], q_corner.at[1]),
        }
    )
    if away:
        moves["shift0"] = (steps, 0, total.at[0], main.at[0])
        moves["shift1"] = (steps, 0, total.at[end], main.at[end])
        moves["shift2"] = (steps, 0, total.at[mid], main.at[mid])
    if light:
        moves["halo0"] = (steps, -1, put.at[0], halo.at[1])
        moves["halo1"] = (steps, 1, put.at[end], halo.at[0])
    else:
        moves["halo0"] = (0, -1, main.at[0], halo.at[1])
        moves["halo1"] = (0, 1, main.at[end], halo.at[0])

    def device(east, north):
        return {
            "lon": lax.rem(lax.axis_index("lon") + n_lon + east, n_lon),
            "band": lax.rem(lax.axis_index("band") + n_band + north, n_band),
        }

    barrier = pltpu.get_barrier_semaphore()
    near = sorted({(east % n_lon, north) for east, north, _, _ in moves.values()})
    for east, north in near:
        pl.semaphore_signal(barrier, inc=1, device_id=device(-east, -north), device_id_type=MESH)

    reads = [
        pltpu.make_async_copy(source, target, read.at[i])
        for i, (source, target) in enumerate(
            ((area, area_in), (parent, parent_in), (relax, relax_in), (zonal, zonal_in), (merid, merid_in))
        )
    ]
    parts = 4
    rows_of = nest.shape[0] // parts

    def nest_part(i):
        here = pl.ds(pl.multiple_of(i * rows_of, 8), rows_of)
        return pltpu.make_async_copy(nest.at[here], nest_in.at[here], read.at[len(reads) + i])

    reads[0].start()
    for i in range(parts):
        nest_part(i).start()
    for copy in reads[1:]:
        copy.start()

    shape = (FRAME + 2 * HALF, width)
    row = lax.broadcasted_iota(jnp.int32, shape, 0)
    shift = jnp.where(
        row < FRAME,
        NS,
        jnp.where(row < FRAME + HALF, FRAME + NS - par_cols, 2 * HALF + NS + par_cols),
    )
    gap = lax.broadcasted_iota(jnp.int32, shape, 1) + (offset[0] - width * steps) - 3 * (row - shift)
    chosen[...] = ((gap >= 0) & (gap < 3)).astype(jnp.float32).astype(jnp.bfloat16)

    spans = [(at, min(LANES, width - at)) for at in range(0, width, LANES)]
    reads[0].wait()
    for t, (at, span) in enumerate(spans):
        area_tiles[t, :, 0:span] = area_in[:, at : at + span]
    area_sums = jnp.concatenate(
        [
            sum(area_tiles[t, pl.ds(i, par_rows, 3), :] for i in range(3))[:, :span]
            for t, (_, span) in enumerate(spans)
        ],
        axis=1,
    )
    spread = product(pieces(area_sums, 3), [chosen[...]])
    spread = jnp.concatenate([spread, jnp.zeros((par_rows, 2 * LANES - shape[0]), jnp.float32)], axis=1)
    lane = lax.broadcasted_iota(jnp.int32, (par_rows, LANES), 1)
    zero = jnp.zeros((par_rows, LANES), jnp.float32)

    def window(start, first, count):
        turned = pltpu.roll(spread, (first - start) % (2 * LANES), 1)[:, :LANES]
        return jnp.where((lane >= first) & (lane < first + count), turned, zero)

    for target, at, here in (
        (x_own, FRAME, window(0, 0, FRAME)),
        (x_side.at[0], HALF, window(FRAME, 0, HALF)),
        (x_side.at[1], HALF, window(FRAME + HALF, FRAME - HALF, HALF)),
    ):
        for block in range(blocks):
            tile = 8 * (per * block // 8)
            target[block, at : at + 8, :] = here[tile : tile + 8]

    def weigh_part(i, carry):
        nest_part(i).wait()

        def weigh(level, inside):
            rows = pl.ds(pl.multiple_of(i * rows_of + level * nest_rows, 8), nest_rows)
            for t, (at, span) in enumerate(spans):
                tiles[t, rows, 0:span] = nest_in[rows, at : at + span] * area_in[:, at : at + span]
            return inside

        return lax.fori_loop(0, levels // parts, weigh, carry)

    lax.fori_loop(0, parts, weigh_part, 0)
    for copy in reads[1:]:
        copy.wait()
    plain[:, 0:par_cols] = parent_in[...]

    def gather(r, carry):
        here = pl.ds(pl.multiple_of(levels * r, levels), levels)
        for t, (at, span) in enumerate(spans):
            sums[here, at : at + span] = sum(
                tiles[t, pl.ds(3 * r + i, levels, nest_rows), :] for i in range(3)
            )[:, :span]
        cells[here, :] = plain[pl.ds(r, levels, par_rows), :]
        return carry

    lax.fori_loop(0, par_rows, gather, 0)
    edge_row = lax.broadcasted_iota(jnp.int32, (16, par_cols), 0)
    edge_col = lax.broadcasted_iota(jnp.int32, (16, par_cols), 1)
    wanted = jnp.where(edge_row < 8, edge_row, edge_row + par_cols - 16)
    ends = (edge_col == wanted).astype(jnp.float32).astype(jnp.bfloat16)

    def spread_pair(pair, carry):
        here = pl.ds(pl.multiple_of(2 * LANES * pair, 2 * LANES), 2 * LANES)
        spread = product([chosen[...]], pieces(sums[here, :], 2))
        outer = product([ends], pieces(cells[here, 0:par_cols], 3))
        for k in range(2):
            block, part = 2 * pair + k, slice(LANES * k, LANES * (k + 1))
            x_own[block, :FRAME, :] = spread[:FRAME, part]
            x_side[0, block, :HALF, :] = spread[FRAME : FRAME + HALF, part]
            x_side[1, block, :HALF, :] = spread[FRAME + HALF :, part]
            p_edge[block, :, :] = outer[:, part]
        return carry

    lax.fori_loop(0, blocks // 2, spread_pair, 0)

    copies = {
        name: pltpu.make_async_remote_copy(
            source, target, sent.at[i], came.at[i], device_id=device(east, north), device_id_type=MESH
        )
        for i, (name, (east, north, source, target)) in enumerate(moves.items())
    }
    pl.semaphore_wait(barrier, len(near))
    early = [name for name in copies if not name.startswith(("corner", "shift", "halo"))]
    for name in early:
        copies[name].start()
    for k, values in enumerate((relax_in, zonal_in, merid_in)):
        upright = jnp.broadcast_to(values[...], (LANES, levels)).T
        weights[levels * k : levels * (k + 1), :] = upright

    waiting = list(copies)

    def arrived(*names):
        for name in names:
            copies[name].wait_recv()
            waiting.remove(name)

    def add(block):
        put[block] = x_own[block]
        put[block, 0:HALF, :] += r_side[0, block, :HALF, :]
        put[block, FRAME - HALF : FRAME, :] += r_side[1, block, :HALF, :]
        put[block, FRAME:, :] += r_side[0, block, HALF:, :] + r_side[1, block, HALF:, :]

    def go(*names):
        for name in names:
            if name in copies:
                copies[name].start()

    arrived("carry0", "carry1")
    add(0)
    if light:
        go("halo0")
    go("shift0")
    arrived("carry2", "carry3")
    add(end)
    if light:
        go("halo1")
    go("shift1")
    arrived("carry4", "carry5")
    for block in range(1, end):
        add(block)
    go("shift2")
    arrived("edge0", "edge1")
    go("corner0", "corner1")
    if not light:
        arrived("shift0")
        go("halo0")
        arrived("shift1")
        go("halo1")
    arrived(*list(waiting))
    for copy in copies.values():
        copy.wait_send()


def smooth_kernel(
    n_band, main, halo, q_edge, q_corner, q_rows, cells, weights, out, field, other, plain
):
    levels = 32
    par_rows = cells.shape[0] // levels
    par_cols = out.shape[1]
    band = lax.axis_index("band")
    weight = [weights[levels * k : levels * (k + 1), :] for k in range(3)]
    lane = lax.broadcasted_iota(jnp.int32, (levels, LANES), 1)
    per = LANES // levels
    gap = jnp.zeros((LANES - 16 - FRAME, LANES), jnp.float32)

    def blend(sums, edges, first, wanted):
        inverse = 1.0 / sums[FRAME:]
        natural = jnp.concatenate([sums[:FRAME], edges[8:16], gap, edges[0:8]], axis=0).T
        for k, own, r in wanted:
            area_row = inverse[first + k : first + k + 1, :]
            got = natural[levels * k : levels * (k + 1), :]
            base = jnp.where(
                lane < par_cols + NS,
                pltpu.roll(jnp.where(lane < par_cols, own(), got), NS, 1),
                pltpu.roll(got, LANES + par_cols + NS - FRAME, 1),
            )
            field[levels * r : levels * (r + 1), :] = base + weight[0] * (got * area_row - base)

    blend(
        halo[0], q_corner[0], 8 - per,
        [
            (per - NS + k, lambda k=k: q_rows[0, levels * k : levels * (k + 1), :], k)
            for k in range(NS)
        ],
    )
    for block in range(par_rows // per):
        blend(
            main[block], q_edge[block], per * block % 8,
            [
                (r % per, lambda r=r: cells[levels * r : levels * (r + 1), :], NS + r)
                for r in range(per * block, per * (block + 1))
            ],
        )
    blend(
        halo[1], q_corner[1], 0,
        [
            (k, lambda k=k: q_rows[1, levels * k : levels * (k + 1), :], NS + par_rows + k)
            for k in range(NS)
        ],
    )
    rows = par_rows + 2 * NS

    def load(ref, r):
        value = ref[levels * r : levels * (r + 1), :]
        if r < NS:
            value = jnp.where(band > 0, value, 0.0)
        if r >= NS + par_rows:
            value = jnp.where(band < n_band - 1, value, 0.0)
        return value

    refs = [field, other]
    for sweep in range(NS):
        read, write = refs[sweep % 2], refs[1 - sweep % 2]
        zoned = {}
        for r in range(sweep, rows - sweep):
            value = load(read, r)
            zoned[r] = value + weight[1] * (
                pltpu.roll(value, 1, 1) - 2.0 * value + pltpu.roll(value, LANES - 1, 1)
            )
            if r >= sweep + 2:
                middle = zoned[r - 1]
                result = middle + weight[2] * (zoned[r - 2] - 2.0 * middle + zoned[r])
                if sweep < NS - 1:
                    write[levels * (r - 1) : levels * r, :] = result
                else:
                    plain[pl.ds(r - 1 - NS, levels, par_rows), :] = pltpu.roll(result, LANES - NS, 1)
    out[...] = plain[:, 0:par_cols]


def on_device(nest_field, nest_area, parent_field, nest_offset, relax_rate, zonal_coef, merid_coef):
    levels, par_rows, par_cols = parent_field.shape
    n_lon, n_band = lax.axis_size("lon"), lax.axis_size("band")
    width = nest_field.shape[2]
    total = levels * par_rows
    f32 = jnp.float32
    nest = nest_field.reshape(-1, width)
    parent = parent_field.reshape(total, par_cols)

    def shaped(*shape):
        return jax.ShapeDtypeStruct(shape, f32)

    blocks = total // LANES
    spans = -(-width // LANES)

    def route(steps):
        return pl.pallas_call(
            functools.partial(route_kernel, steps, n_lon, n_band),
            name="route%d" % steps,
            out_shape=[
                shaped(blocks, FRAME + 8, LANES),
                shaped(2, FRAME + 8, LANES),
                shaped(blocks, 16, LANES),
                shaped(2, 16, LANES),
                shaped(2, levels * NS, LANES),
                shaped(total, LANES),
                shaped(3 * levels, LANES),
            ],
            in_specs=[SMEM] + [pl.BlockSpec(memory_space=pl.ANY)] * 6,
            out_specs=[VMEM] * 7,
            scratch_shapes=[
                pltpu.VMEM(nest.shape, f32),
                pltpu.VMEM(nest_area.shape, f32),
                pltpu.VMEM(parent.shape, f32),
                pltpu.VMEM((1, levels), f32),
                pltpu.VMEM((1, levels), f32),
                pltpu.VMEM((1, levels), f32),
                pltpu.VMEM((spans, nest.shape[0], LANES), f32),
                pltpu.VMEM((spans, nest_area.shape[0], LANES), f32),
                pltpu.VMEM((total, width), f32),
                pltpu.VMEM((total, LANES), f32),
                pltpu.VMEM((FRAME + 2 * HALF, width), jnp.bfloat16),
                pltpu.VMEM((blocks, FRAME + 8, LANES), f32),
                pltpu.VMEM((2, blocks, HALF + 8, LANES), f32),
                pltpu.VMEM((blocks, 16, LANES), f32),
                pltpu.VMEM((2, blocks, HALF + 8, LANES), f32),
                pltpu.VMEM((blocks, FRAME + 8, LANES), f32),
                pltpu.SemaphoreType.DMA((17,)),
                pltpu.SemaphoreType.DMA((17,)),
                pltpu.SemaphoreType.DMA((9,)),
            ],
            compiler_params=pltpu.CompilerParams(collective_id=steps, has_side_effects=True),
        )

    routes = [lambda *values, steps=steps: route(steps)(*values) for steps in range(1, n_lon + 1)]
    moved = lax.switch(
        (nest_offset[0] + width // 2) // width - 1,
        routes,
        nest_offset, nest, nest_area, parent,
        relax_rate.reshape(1, levels), zonal_coef.reshape(1, levels), merid_coef.reshape(1, levels),
    )
    rows = levels * (par_rows + 2 * NS)
    out = pl.pallas_call(
        functools.partial(smooth_kernel, n_band),
        name="smooth",
        out_shape=shaped(total, par_cols),
        in_specs=[VMEM] * 7,
        out_specs=VMEM,
        scratch_shapes=[
            pltpu.VMEM((rows, LANES), f32),
            pltpu.VMEM((rows, LANES), f32),
            pltpu.VMEM((total, LANES), f32),
        ],
    )(*moved)
    return out.reshape(levels, par_rows, par_cols)


def solution(mesh):
    placed = (P(None, "band", "lon"), P("band", "lon"), P(None, "band", "lon"), P(), P(), P(), P())
    return jax.shard_map(
        on_device, mesh=mesh, in_specs=placed, out_specs=P(None, "band", "lon"), check_vma=False
    )
```

```python
import functools

import jax
import jax.numpy as jnp
from jax import lax
from jax.experimental import pallas as pl
from jax.experimental.pallas import tpu as pltpu
from jax.sharding import PartitionSpec as P

NS = 3
FRAME = 104
LANES = 128
RING = 8
LIGHT = 2
HALF = 56
SIDE = HALF + 8
MESH = pl.DeviceIdType.MESH
VMEM = pl.BlockSpec(memory_space=pltpu.VMEM)
SMEM = pl.BlockSpec(memory_space=pltpu.SMEM)


def pieces(value, count):
    found = []
    for _ in range(count):
        piece = value.astype(jnp.bfloat16)
        value = value - piece.astype(jnp.float32)
        found.append(piece)
    return found


def product(left_pieces, right_pieces):
    total = None
    for left in left_pieces:
        for right in right_pieces:
            part = lax.dot_general(
                left, right, (((1,), (1,)), ((), ())), preferred_element_type=jnp.float32
            )
            total = part if total is None else total + part
    return total


def route_kernel(
    steps, n_lon, n_band, offset, nest, area, parent, relax, zonal, merid,
    main, halo, q_edge, q_corner, q_rows, cells, weights,
    nest_in, area_in, parent_in, relax_in, zonal_in, merid_in, tiles, area_tiles, sums, plain, chosen,
    x_own, x_side, p_edge, r_side, total, sent, came, read,
):
    levels, width, par_cols = 32, nest.shape[1], parent.shape[1]
    par_rows = parent.shape[0] // levels
    nest_rows = 3 * par_rows
    per = LANES // levels
    blocks = par_rows // per
    end, mid = blocks - 1, pl.ds(1, blocks - 2)
    low, high = pl.ds(0, 8), pl.ds(8, 8)
    columns = levels * par_rows
    hops = [(steps + core) // 2 % RING for core in range(2)]
    load = sum(min(hop, RING - hop) for hop in hops)
    light = load <= LIGHT
    away = steps % n_lon
    put = total if away else main
    moves = {}
    for k, east in enumerate((1, -1)):
        for i, (block, count) in enumerate(((0, SIDE), (end, SIDE), (mid, HALF))):
            here = pl.ds(SIDE * k, count)
            moves["carry%d" % (2 * i + k)] = (east, 0, x_side.at[block, here], r_side.at[block, here])
    moves = {name: moves[name] for name in sorted(moves)}
    moves.update(
        {
            "edge0": (1, 0, p_edge.at[:, high], q_edge.at[:, low]),
            "edge1": (-1, 0, p_edge.at[:, low], q_edge.at[:, high]),
            "row0": (0, 1, cells.at[pl.ds(columns - levels * NS, levels * NS)], q_rows.at[0]),
            "row1": (0, -1, cells.at[pl.ds(0, levels * NS)], q_rows.at[1]),
            "corner0": (0, 1, q_edge.at[end], q_corner.at[0]),
            "corner1": (0, -1, q_edge.at[0], q_corner.at[1]),
        }
    )
    if away:
        moves["shift0"] = (steps, 0, total.at[0], main.at[0])
        moves["shift1"] = (steps, 0, total.at[end], main.at[end])
        moves["shift2"] = (steps, 0, total.at[mid, pl.ds(0, FRAME)], main.at[mid, pl.ds(0, FRAME)])
    if light:
        moves["halo0"] = (steps, -1, put.at[0], halo.at[1])
        moves["halo1"] = (steps, 1, put.at[end], halo.at[0])
    else:
        moves["halo0"] = (0, -1, main.at[0], halo.at[1])
        moves["halo1"] = (0, 1, main.at[end], halo.at[0])

    def device(east, north):
        return {
            "lon": lax.rem(lax.axis_index("lon") + n_lon + east, n_lon),
            "band": lax.rem(lax.axis_index("band") + n_band + north, n_band),
        }

    barrier = pltpu.get_barrier_semaphore()
    near = sorted({(east % n_lon, north) for east, north, _, _ in moves.values()})
    for east, north in near:
        pl.semaphore_signal(barrier, inc=1, device_id=device(-east, -north), device_id_type=MESH)

    reads = [
        pltpu.make_async_copy(source, target, read.at[i])
        for i, (source, target) in enumerate(
            ((area, area_in), (parent, parent_in), (relax, relax_in), (zonal, zonal_in), (merid, merid_in))
        )
    ]
    parts = 4
    rows_of = nest.shape[0] // parts

    def nest_part(i):
        here = pl.ds(pl.multiple_of(i * rows_of, 8), rows_of)
        return pltpu.make_async_copy(nest.at[here], nest_in.at[here], read.at[len(reads) + i])

    reads[0].start()
    for i in range(parts):
        nest_part(i).start()
    for copy in reads[1:]:
        copy.start()

    shape = (4 * SIDE, width)
    row = lax.broadcasted_iota(jnp.int32, shape, 0)
    shift = jnp.where(
        row < SIDE,
        NS - par_cols,
        jnp.where(row < 2 * SIDE, SIDE + HALF - FRAME + NS + par_cols, 2 * SIDE + NS),
    )
    gap = lax.broadcasted_iota(jnp.int32, shape, 1) + (offset[0] - width * steps) - 3 * (row - shift)
    chosen[...] = ((gap >= 0) & (gap < 3)).astype(jnp.float32).astype(jnp.bfloat16)

    spans = [(at, min(LANES, width - at)) for at in range(0, width, LANES)]
    reads[0].wait()
    for t, (at, span) in enumerate(spans):
        area_tiles[t, :, 0:span] = area_in[:, at : at + span]
    area_sums = jnp.concatenate(
        [
            sum(area_tiles[t, pl.ds(i, par_rows, 3), :] for i in range(3))[:, :span]
            for t, (_, span) in enumerate(spans)
        ],
        axis=1,
    )
    spread = product(pieces(area_sums, 2), [chosen[...]])
    lane = lax.broadcasted_iota(jnp.int32, (par_rows, LANES), 1)
    zero = jnp.zeros((par_rows, LANES), jnp.float32)

    def window(start, first, count):
        turned = pltpu.roll(spread, (first - start) % (2 * LANES), 1)[:, :LANES]
        return jnp.where((lane >= first) & (lane < first + count), turned, zero)

    for target, at, here in (
        (x_own, FRAME, window(2 * SIDE, 0, FRAME)),
        (x_side, HALF, window(0, 0, HALF)),
        (x_side, SIDE + HALF, window(SIDE, FRAME - HALF, HALF)),
    ):
        target[0, at : at + 8, :] = here[0:8]
        target[end, at : at + 8, :] = here[8:16]

    def weigh_part(i, carry):
        nest_part(i).wait()

        def weigh(level, inside):
            rows = pl.ds(pl.multiple_of(i * rows_of + level * nest_rows, 8), nest_rows)
            for t, (at, span) in enumerate(spans):
                tiles[t, rows, 0:span] = nest_in[rows, at : at + span] * area_in[:, at : at + span]
            return inside

        return lax.fori_loop(0, levels // parts, weigh, carry)

    lax.fori_loop(0, parts, weigh_part, 0)
    def gather(r, carry):
        here = pl.ds(pl.multiple_of(levels * r, levels), levels)
        for t, (at, span) in enumerate(spans):
            sums[here, at : at + span] = sum(
                tiles[t, pl.ds(3 * r + i, levels, nest_rows), :] for i in range(3)
            )[:, :span]
        return carry

    lax.fori_loop(0, par_rows, gather, 0)

    def spread_side(pair, carry):
        here = pl.ds(pl.multiple_of(2 * LANES * pair, 2 * LANES), 2 * LANES)
        spread = product([chosen[: 2 * SIDE]], pieces(sums[here, :], 2))
        for k in range(2):
            part = slice(LANES * k, LANES * (k + 1))
            x_side[2 * pair + k, :HALF, :] = spread[:HALF, part]
            x_side[2 * pair + k, SIDE : SIDE + HALF, :] = spread[SIDE : SIDE + HALF, part]
        return carry

    lax.fori_loop(0, blocks // 2, spread_side, 0)
    copies = {
        name: pltpu.make_async_remote_copy(
            source, target, sent.at[i], came.at[i], device_id=device(east, north), device_id_type=MESH
        )
        for i, (name, (east, north, source, target)) in enumerate(moves.items())
    }
    pl.semaphore_wait(barrier, len(near))
    for name in copies:
        if name.startswith("carry"):
            copies[name].start()
    for copy in reads[1:]:
        copy.wait()
    plain[:, 0:par_cols] = parent_in[...]

    def turn(r, carry):
        here = pl.ds(pl.multiple_of(levels * r, levels), levels)
        cells[here, :] = plain[pl.ds(r, levels, par_rows), :]
        return carry

    lax.fori_loop(0, par_rows, turn, 0)
    edge_row = lax.broadcasted_iota(jnp.int32, (16, par_cols), 0)
    edge_col = lax.broadcasted_iota(jnp.int32, (16, par_cols), 1)
    wanted = jnp.where(edge_row < 8, edge_row, edge_row + par_cols - 16)
    ends = (edge_col == wanted).astype(jnp.float32).astype(jnp.bfloat16)

    def spread_own(pair, carry):
        here = pl.ds(pl.multiple_of(2 * LANES * pair, 2 * LANES), 2 * LANES)
        spread = product([chosen[2 * SIDE :]], pieces(sums[here, :], 2))
        outer = product([ends], pieces(cells[here, 0:par_cols], 2))
        for k in range(2):
            block, part = 2 * pair + k, slice(LANES * k, LANES * (k + 1))
            x_own[block, :FRAME, :] = spread[:FRAME, part]
            p_edge[block, :, :] = outer[:, part]
        return carry

    lax.fori_loop(0, blocks // 2, spread_own, 0)
    for name in copies:
        if name.startswith(("edge", "row")):
            copies[name].start()
    for k, values in enumerate((relax_in, zonal_in, merid_in)):
        upright = jnp.broadcast_to(values[...], (LANES, levels)).T
        weights[levels * k : levels * (k + 1), :] = upright

    waiting = list(copies)

    def arrived(*names):
        for name in names:
            copies[name].wait_recv()
            waiting.remove(name)

    def add(block):
        put[block] = x_own[block, : FRAME + 8]
        put[block, 0:HALF, :] += r_side[block, :HALF, :]
        put[block, FRAME - HALF : FRAME, :] += r_side[block, SIDE : SIDE + HALF, :]
        if block in (0, end):
            put[block, FRAME:, :] += r_side[block, HALF:SIDE, :] + r_side[block, SIDE + HALF :, :]

    def go(*names):
        for name in names:
            if name in copies:
                copies[name].start()

    arrived("carry0", "carry1")
    add(0)
    if light:
        go("halo0")
    go("shift0")
    arrived("carry2", "carry3")
    add(end)
    if light:
        go("halo1")
    go("shift1")
    arrived("carry4", "carry5")
    for block in range(1, end):
        add(block)
    go("shift2")
    arrived("edge0", "edge1")
    go("corner0", "corner1")
    if not light:
        arrived("shift0")
        go("halo0")
        arrived("shift1")
        go("halo1")
    arrived(*list(waiting))
    for copy in copies.values():
        copy.wait_send()


def smooth_kernel(
    n_band, main, halo, q_edge, q_corner, q_rows, cells, weights, out, field, other, plain
):
    levels = 32
    par_rows = cells.shape[0] // levels
    par_cols = out.shape[1]
    band = lax.axis_index("band")
    weight = [weights[levels * k : levels * (k + 1), :] for k in range(3)]
    lane = lax.broadcasted_iota(jnp.int32, (levels, LANES), 1)
    per = LANES // levels
    gap = jnp.zeros((LANES - 16 - FRAME, LANES), jnp.float32)

    def blend(sums, areas, edges, first, wanted):
        inverse = 1.0 / areas[FRAME:]
        natural = jnp.concatenate([sums[:FRAME], edges[8:16], gap, edges[0:8]], axis=0).T
        for k, own, r in wanted:
            area_row = inverse[first + k : first + k + 1, :]
            got = natural[levels * k : levels * (k + 1), :]
            base = jnp.where(
                lane < par_cols + NS,
                pltpu.roll(jnp.where(lane < par_cols, own(), got), NS, 1),
                pltpu.roll(got, LANES + par_cols + NS - FRAME, 1),
            )
            field[levels * r : levels * (r + 1), :] = base + weight[0] * (got * area_row - base)

    blend(
        halo[0], halo[0], q_corner[0], 8 - per,
        [
            (per - NS + k, lambda k=k: q_rows[0, levels * k : levels * (k + 1), :], k)
            for k in range(NS)
        ],
    )
    for block in range(par_rows // per):
        blend(
            main[block], main[0 if per * block < 8 else par_rows // per - 1], q_edge[block], per * block % 8,
            [
                (r % per, lambda r=r: cells[levels * r : levels * (r + 1), :], NS + r)
                for r in range(per * block, per * (block + 1))
            ],
        )
    blend(
        halo[1], halo[1], q_corner[1], 0,
        [
            (k, lambda k=k: q_rows[1, levels * k : levels * (k + 1), :], NS + par_rows + k)
            for k in range(NS)
        ],
    )
    rows = par_rows + 2 * NS

    def load(ref, r):
        value = ref[levels * r : levels * (r + 1), :]
        if r < NS:
            value = jnp.where(band > 0, value, 0.0)
        if r >= NS + par_rows:
            value = jnp.where(band < n_band - 1, value, 0.0)
        return value

    refs = [field, other]
    for sweep in range(NS):
        read, write = refs[sweep % 2], refs[1 - sweep % 2]
        zoned = {}
        for r in range(sweep, rows - sweep):
            value = load(read, r)
            zoned[r] = value + weight[1] * (
                pltpu.roll(value, 1, 1) - 2.0 * value + pltpu.roll(value, LANES - 1, 1)
            )
            if r >= sweep + 2:
                middle = zoned[r - 1]
                result = middle + weight[2] * (zoned[r - 2] - 2.0 * middle + zoned[r])
                if sweep < NS - 1:
                    write[levels * (r - 1) : levels * r, :] = result
                else:
                    plain[pl.ds(r - 1 - NS, levels, par_rows), :] = pltpu.roll(result, LANES - NS, 1)
    out[...] = plain[:, 0:par_cols]


def on_device(nest_field, nest_area, parent_field, nest_offset, relax_rate, zonal_coef, merid_coef):
    levels, par_rows, par_cols = parent_field.shape
    n_lon, n_band = lax.axis_size("lon"), lax.axis_size("band")
    width = nest_field.shape[2]
    total = levels * par_rows
    f32 = jnp.float32
    nest = nest_field.reshape(-1, width)
    parent = parent_field.reshape(total, par_cols)

    def shaped(*shape):
        return jax.ShapeDtypeStruct(shape, f32)

    blocks = total // LANES
    spans = -(-width // LANES)

    def route(steps):
        return pl.pallas_call(
            functools.partial(route_kernel, steps, n_lon, n_band),
            name="route%d" % steps,
            out_shape=[
                shaped(blocks, FRAME + 8, LANES),
                shaped(2, FRAME + 8, LANES),
                shaped(blocks, 16, LANES),
                shaped(2, 16, LANES),
                shaped(2, levels * NS, LANES),
                shaped(total, LANES),
                shaped(3 * levels, LANES),
            ],
            in_specs=[SMEM] + [pl.BlockSpec(memory_space=pl.ANY)] * 6,
            out_specs=[VMEM] * 7,
            scratch_shapes=[
                pltpu.VMEM(nest.shape, f32),
                pltpu.VMEM(nest_area.shape, f32),
                pltpu.VMEM(parent.shape, f32),
                pltpu.VMEM((1, levels), f32),
                pltpu.VMEM((1, levels), f32),
                pltpu.VMEM((1, levels), f32),
                pltpu.VMEM((spans, nest.shape[0], LANES), f32),
                pltpu.VMEM((spans, nest_area.shape[0], LANES), f32),
                pltpu.VMEM((total, width), f32),
                pltpu.VMEM((total, LANES), f32),
                pltpu.VMEM((4 * SIDE, width), jnp.bfloat16),
                pltpu.VMEM((blocks, 2 * SIDE, LANES), f32),
                pltpu.VMEM((blocks, 2 * SIDE, LANES), f32),
                pltpu.VMEM((blocks, 16, LANES), f32),
                pltpu.VMEM((blocks, 2 * SIDE, LANES), f32),
                pltpu.VMEM((blocks, FRAME + 8, LANES), f32),
                pltpu.SemaphoreType.DMA((17,)),
                pltpu.SemaphoreType.DMA((17,)),
                pltpu.SemaphoreType.DMA((9,)),
            ],
            compiler_params=pltpu.CompilerParams(collective_id=steps, has_side_effects=True),
        )

    routes = [lambda *values, steps=steps: route(steps)(*values) for steps in range(1, n_lon + 1)]
    moved = lax.switch(
        (nest_offset[0] + width // 2) // width - 1,
        routes,
        nest_offset, nest, nest_area, parent,
        relax_rate.reshape(1, levels), zonal_coef.reshape(1, levels), merid_coef.reshape(1, levels),
    )
    rows = levels * (par_rows + 2 * NS)
    out = pl.pallas_call(
        functools.partial(smooth_kernel, n_band),
        name="smooth",
        out_shape=shaped(total, par_cols),
        in_specs=[VMEM] * 7,
        out_specs=VMEM,
        scratch_shapes=[
            pltpu.VMEM((rows, LANES), f32),
            pltpu.VMEM((rows, LANES), f32),
            pltpu.VMEM((total, LANES), f32),
        ],
    )(*moved)
    return out.reshape(levels, par_rows, par_cols)


def solution(mesh):
    placed = (P(None, "band", "lon"), P("band", "lon"), P(None, "band", "lon"), P(), P(), P(), P())
    return jax.shard_map(
        on_device, mesh=mesh, in_specs=placed, out_specs=P(None, "band", "lon"), check_vma=False
    )
```
